32 devices in a mesh: pb: 4 (over x, core), ka: 8 (over z, y).
Axes of the slice: x: 2, y: 2, z: 4, core: 2. Of those that a mesh axis runs over, the one named last changes fastest.
Arguments:
- queries: bfloat16 [4096, 1024], P(('pb', 'ka')), may hold values from -6 to 6
- key_rows: bfloat16 [4096, 128], P(('pb', 'ka')), may hold values from -6 to 6
- value_rows: bfloat16 [4096, 128], P(('pb', 'ka')), may hold values from -6 to 6
- forward_out: bfloat16 [4096, 1024], P(('pb', 'ka')), may hold values from -6 to 6
- out_grad: bfloat16 [4096, 1024], P(('pb', 'ka')), may hold values from -4 to 4
- logsumexp: float32 [8, 4096], P(None, ('pb', 'ka')), may hold values from 3 to 7
- position: int32 [4096], P(('pb', 'ka')), may hold values from 0 to 4095, as said below
- segment: int32 [4096], P(('pb', 'ka')), may hold values from 0 to 7, as said below
Outputs:
- query_grad: bfloat16 [4096, 1024], P(('pb', 'ka'))
- key_grad: bfloat16 [4096, 128], P(('pb', 'ka'))
- value_grad: bfloat16 [4096, 128], P(('pb', 'ka'))
The draws below stay inside these ranges and needn't reach their ends.
Inputs may be any that keep to these rules, and one draw needn't show every extreme that they name: `position`: a permutation of 0 to 4095; each aligned run of 128 rows holds 128 consecutive positions in increasing order. `segment`: the document of the row's position; each document is a nonempty run of consecutive positions, numbered in the order of positions, 8 documents in all.
All inputs are finite; a program needn't handle non-finite values.
Results may differ from the reference program's by a relative error of at most 0.0051.
Values may be sent and summed in bfloat16 or wider, within the bound.
No kernel may reach another device: no remote copies, remote signals or barrier semaphores. Data moves between devices by JAX's collectives and lax.ppermute only.
A program may use at most 64 MiB of HBM per device.

```python
import jax
import jax.numpy as jnp
from jax import lax

HEADS = 8
HD = 128
TOK_DEV = 128
DOCS = 8
LENGTH = 4096


def build_layout(key):
    perm_key = jax.random.fold_in(key, 11)
    doc_key = jax.random.fold_in(key, 12)
    block_total = LENGTH // TOK_DEV
    block_order = jax.random.permutation(perm_key, block_total).astype(jnp.int32)
    position = (block_order[:, None] * TOK_DEV + jnp.arange(TOK_DEV, dtype=jnp.int32)[None, :]).reshape(-1).astype(jnp.int32)
    boundaries = (jax.random.choice(doc_key, LENGTH - 1, (DOCS - 1,), replace=False) + 1).astype(jnp.int32)
    document_ids = jnp.sum((jnp.arange(LENGTH, dtype=jnp.int32)[:, None] >= boundaries[None, :]).astype(jnp.int32), axis=1).astype(jnp.int32)
    segment = document_ids[position].astype(jnp.int32)
    return (position, segment)


def draw_position(key, part):
    return build_layout(key)[0]


def draw_segment(key, part):
    return build_layout(key)[1]


def level_of(own_key, dims, shards, least, largest):
    level, own = 1.0, jax.random.fold_in(own_key, 6)
    for dim, blocks in shards:
        steps = jnp.exp(jax.random.uniform(jax.random.fold_in(own, dim), (blocks,), jnp.float32, least / len(shards), largest / len(shards)))
        level = level * jnp.repeat(steps, dims[dim] // blocks).reshape([-1 if axis == dim else 1 for axis in range(len(dims))])
    return level


def centred(stream_key, extent, spread, reach, pieces=(), kind=jnp.bfloat16):
    entries = spread * jax.random.normal(stream_key, extent, jnp.float32)
    if pieces:
        entries = entries * level_of(stream_key, extent, pieces, -0.22, 0.18)
    return jnp.clip(entries, -reach, reach).astype(kind)


def setup_inputs(seed: int = 0) -> dict:
    seeds = jax.random.split(jax.random.key(seed), 9)
    return {
        "queries": centred(seeds[0], (LENGTH, HEADS * HD), 1.0, 6.0, ((0, 32),)),
        "key_rows": centred(seeds[1], (LENGTH, HD), 1.0, 6.0, ((0, 32),)),
        "value_rows": centred(seeds[2], (LENGTH, HD), 1.0, 6.0, ((0, 32),)),
        "forward_out": centred(seeds[3], (LENGTH, HEADS * HD), 0.5, 6.0, ((0, 32),)),
        "out_grad": centred(seeds[4], (LENGTH, HEADS * HD), 0.25, 4.0, ((0, 32),)),
        "logsumexp": jnp.clip(3.0 + 4.0 * jax.random.uniform(seeds[5], (HEADS, LENGTH), jnp.float32) ** level_of(seeds[5], (HEADS, LENGTH), ((1, 32),), -0.2, 0.2), 3.0, 7.0),
        "position": draw_position(jax.random.fold_in(seeds[8], 71), 0),
        "segment": draw_segment(jax.random.fold_in(seeds[8], 71), 0),
    }


def reference(queries, key_rows, value_rows, forward_out, out_grad, logsumexp, position, segment):
    head_width = key_rows.shape[1]
    row_count = queries.shape[0]
    head_count = queries.shape[1] // head_width
    score_scale = head_width ** -0.5
    highest = lax.Precision.HIGHEST
    delta_rows = jnp.sum((out_grad.astype(jnp.float32) * forward_out.astype(jnp.float32)).reshape(row_count, head_count, head_width), axis=2).T
    block_rows = min(512, row_count)
    block_count = row_count // block_rows
    key_float = key_rows.astype(jnp.float32)
    value_float = value_rows.astype(jnp.float32)

    def scan_step(loop_state, block_index):
        key_acc, value_acc = loop_state
        first_row = (block_index * block_rows).astype(jnp.int32)
        query_tile = lax.dynamic_slice_in_dim(queries, first_row, block_rows, 0).astype(jnp.float32).reshape(block_rows, head_count, head_width)
        grad_tile = lax.dynamic_slice_in_dim(out_grad, first_row, block_rows, 0).astype(jnp.float32).reshape(block_rows, head_count, head_width)
        lse_tile = lax.dynamic_slice_in_dim(logsumexp, first_row, block_rows, 1)
        delta_tile = lax.dynamic_slice_in_dim(delta_rows, first_row, block_rows, 1)
        place_tile = lax.dynamic_slice_in_dim(position, first_row, block_rows, 0)
        doc_tile = lax.dynamic_slice_in_dim(segment, first_row, block_rows, 0)
        visible = (position[None, :] <= place_tile[:, None]) & (segment[None, :] == doc_tile[:, None])
        scores = jnp.einsum("qhd,kd->hqk", query_tile, key_float, precision=highest) * score_scale
        weights = jnp.where(visible[None], jnp.exp(scores - lse_tile[:, :, None]), 0.0)
        rounded = lax.optimization_barrier(weights.astype(jnp.bfloat16)).astype(jnp.float32)
        value_acc = value_acc + jnp.einsum("hqk,qhd->kd", rounded, grad_tile, precision=highest)
        grad_scores = jnp.einsum("qhd,kd->hqk", grad_tile, value_float, precision=highest)
        score_grads = lax.optimization_barrier((weights * (grad_scores - delta_tile[:, :, None])).astype(jnp.bfloat16)).astype(jnp.float32)
        query_part = jnp.einsum("hqk,kd->qhd", score_grads, key_float, precision=highest).reshape(block_rows, head_count * head_width) * score_scale
        key_acc = key_acc + jnp.einsum("hqk,qhd->kd", score_grads, query_tile, precision=highest)
        return (key_acc, value_acc), query_part.astype(jnp.bfloat16)

    starting = (jnp.zeros((row_count, head_width), jnp.float32), jnp.zeros((row_count, head_width), jnp.float32))
    (key_acc, value_acc), grad_blocks = lax.scan(scan_step, starting, jnp.arange(block_count, dtype=jnp.int32))
    query_grad = grad_blocks.reshape(row_count, head_count * head_width)
    return query_grad, (key_acc * score_scale).astype(jnp.bfloat16), value_acc.astype(jnp.bfloat16)
```

```python
import math

import jax
import jax.numpy as jnp
from jax import lax
from jax.experimental import pallas as pl
from jax.experimental.pallas import tpu as pltpu
from jax.sharding import PartitionSpec as P

AXES = ("pb", "ka")
META = 16
LOG2E = math.log2(math.e)


def nt_dot(left, right):
    return lax.dot_general(
        left, right, (((1,), (1,)), ((), ())), preferred_element_type=jnp.float32
    )


def nn_dot(left, right):
    return lax.dot_general(
        left, right, (((1,), (0,)), ((), ())), preferred_element_type=jnp.float32
    )


def pack_kernel(key, value, place, doc, out):
    rows = key.shape[0]
    out[0, :rows, :] = key[...]
    out[0, rows : 2 * rows, :] = value[...]
    index = lax.broadcasted_iota(jnp.int32, (META, rows), 0)
    block = place[0:1, 0:1] // rows
    meta = jnp.where(index == 0, doc[...], block).astype(jnp.float32)
    out[0, 2 * rows :, :] = meta.astype(out.dtype)


def pack(key, value, place, doc):
    rows, head = key.shape
    return pl.pallas_call(
        pack_kernel,
        out_shape=jax.ShapeDtypeStruct((1, 2 * rows + META, head), key.dtype),
        name="pack_rows",
    )(key, value, place, doc)


def stats_kernel(grad, forward, lse, place, doc, out):
    heads, rows = lse.shape
    head = grad.shape[1] // heads
    for h in range(heads):
        part = slice(h * head, (h + 1) * head)
        product = grad[:, part].astype(jnp.float32) * forward[:, part].astype(jnp.float32)
        spot = slice(h * rows, (h + 1) * rows)
        out[0:1, spot] = lse[h : h + 1, :] * LOG2E
        out[1:2, spot] = jnp.sum(product.T, axis=0, keepdims=True)
        out[2:3, spot] = doc[...].astype(jnp.float32)
        out[3:4, spot] = place[...].astype(jnp.float32)


def row_stats(grad, forward, lse, place, doc):
    heads, rows = lse.shape
    return pl.pallas_call(
        stats_kernel,
        out_shape=jax.ShapeDtypeStruct((4, heads * rows), jnp.float32),
        name="row_stats",
    )(grad, forward, lse, place, doc)


def tile_kernel(
    q_own, q_peer, g_own, g_peer, s_own, s_peer, kv_low, kv_high,
    dq_own, dq_peer, keep, send, qs, gs, dqt, acc, flags, firsts,
):
    rows, width = q_own.shape
    half, span, head = kv_low.shape
    heads = width // head
    scale = head ** (-0.5)
    stats = (s_own, s_peer)
    places = [s[3:4, :rows][0, 0] for s in stats]
    docs = [s[2:3, :rows][0, 0] for s in stats]
    for part, kv in enumerate((kv_low, kv_high)):
        for slot in range(half):
            meta = kv[slot, 2 * rows :, :].astype(jnp.float32)
            first = meta[1, 0] * rows
            firsts[part, slot] = first
            for block in range(2):
                seen = (first <= places[block]) & (meta[0, rows - 1] >= docs[block])
                flags[part, 2 * slot + block] = seen.astype(jnp.int32)
    for block, (q, g) in enumerate(((q_own, g_own), (q_peer, g_peer))):
        for h in range(heads):
            qs[block, h * rows : (h + 1) * rows, :] = q[:, h * head : (h + 1) * head]
            gs[block, h * rows : (h + 1) * rows, :] = g[:, h * head : (h + 1) * head]
    dqt[...] = jnp.zeros_like(dqt)

    for part, (kv, out) in enumerate(((kv_low, keep), (kv_high, send))):

        def over_slots(slot, carry, part=part, kv=kv, out=out):
            acc[...] = jnp.zeros_like(acc)

            for block in range(2):

                @pl.when(flags[part, 2 * slot + block] == 1)
                def _():
                    key = kv[slot, :rows, :]
                    value = kv[slot, rows : 2 * rows, :]
                    doc_row = kv[slot, 2 * rows :, :].astype(jnp.float32)[0:1, :]
                    key_t = key.astype(jnp.float32).T.astype(jnp.bfloat16)
                    doc_col = jnp.broadcast_to(doc_row, (rows, rows)).T[:, 0:1]
                    index = lax.broadcasted_iota(jnp.int32, (rows, 1), 0)
                    place_col = index.astype(jnp.float32) + firsts[part, slot]
                    s = stats[block]
                    visible = (place_col <= s[3:4, :]) & (doc_col == s[2:3, :])
                    scores = nt_dot(key, qs[block])
                    weights = jnp.where(
                        visible, jnp.exp2(scores * (scale * LOG2E) - s[0:1, :]), 0.0
                    )
                    grads = nt_dot(value, gs[block])
                    score_grads = (weights * (grads - s[1:2, :])).astype(jnp.bfloat16)
                    acc[rows:, :] += nn_dot(weights.astype(jnp.bfloat16), gs[block])
                    acc[:rows, :] += nn_dot(score_grads, qs[block])
                    dqt[block] += nn_dot(key_t, score_grads)

            out[slot, :rows, :] = (acc[:rows, :] * scale).astype(out.dtype)
            out[slot, rows:, :] = acc[rows:, :].astype(out.dtype)
            return carry

        lax.fori_loop(0, half, over_slots, 0)
    for block, out in enumerate((dq_own, dq_peer)):
        for h in range(heads):
            out[:, h * head : (h + 1) * head] = (
                dqt[block, :, h * rows : (h + 1) * rows].T * scale
            ).astype(out.dtype)


def tile_grads(q_own, q_peer, g_own, g_peer, s_own, s_peer, kv_low, kv_high):
    rows, width = q_own.shape
    half, _, head = kv_low.shape
    heads = width // head
    return pl.pallas_call(
        tile_kernel,
        out_shape=(
            jax.ShapeDtypeStruct((rows, width), jnp.float32),
            jax.ShapeDtypeStruct((rows, width), jnp.bfloat16),
            jax.ShapeDtypeStruct((half, 2 * rows, head), jnp.float32),
            jax.ShapeDtypeStruct((half, 2 * rows, head), jnp.bfloat16),
        ),
        scratch_shapes=[
            pltpu.VMEM((2, heads * rows, head), jnp.bfloat16),
            pltpu.VMEM((2, heads * rows, head), jnp.bfloat16),
            pltpu.VMEM((2, head, heads * rows), jnp.float32),
            pltpu.VMEM((2 * rows, head), jnp.float32),
            pltpu.SMEM((2, 2 * half), jnp.int32),
            pltpu.SMEM((2, half), jnp.float32),
        ],
        name="tile_grads",
    )(q_own, q_peer, g_own, g_peer, s_own, s_peer, kv_low, kv_high)


def make_body(pb_size, ka_size):
    total = pb_size * ka_size
    core = ka_size
    bits = [1 << b for b in reversed(range(ka_size.bit_length() - 1))]
    bits += [1 << b for b in range(total.bit_length() - 1) if (1 << b) > core]
    orders = (bits, bits[:1] + bits[2:] + bits[1:2])

    def peer(array):
        return lax.ppermute(array, AXES, [(i, i ^ core) for i in range(total)])

    def swap(array, level):
        pairs = [(i, i ^ orders[1 if i & core else 0][level]) for i in range(total)]
        return lax.ppermute(array, AXES, pairs)

    def body(queries, key_rows, value_rows, forward_out, out_grad, logsumexp, position, segment):
        rows = queries.shape[0]
        place, doc = position[None, :], segment[None, :]
        kv = pack(key_rows, value_rows, place, doc)
        stats = row_stats(out_grad, forward_out, logsumexp, place, doc)
        last = len(bits) - 1
        for level in range(last):
            kv = jnp.concatenate([kv, swap(kv, level)])
        kv_high = swap(kv, last)
        q_peer, g_peer, s_peer = peer(queries), peer(out_grad), peer(stats)
        dq_own, dq_send, keep, send = tile_grads(
            queries, q_peer, out_grad, g_peer, stats, s_peer, kv, kv_high
        )
        dq_recv = peer(dq_send)
        for level in reversed(range(len(bits))):
            kept = keep + swap(send, level).astype(jnp.float32)
            if level:
                half = kept.shape[0] // 2
                keep, send = kept[:half], kept[half:].astype(jnp.bfloat16)
        query_grad = (dq_own + dq_recv.astype(jnp.float32)).astype(jnp.bfloat16)
        kept = kept[0].astype(jnp.bfloat16)
        return query_grad, kept[:rows], kept[rows:]

    return body


def solution(mesh):
    placed = (
        P(AXES, None),
        P(AXES, None),
        P(AXES, None),
        P(AXES, None),
        P(AXES, None),
        P(None, AXES),
        P(AXES),
        P(AXES),
    )
    return jax.shard_map(
        make_body(mesh.shape["pb"], mesh.shape["ka"]),
        mesh=mesh,
        in_specs=placed,
        out_specs=(P(AXES, None), P(AXES, None), P(AXES, None)),
        check_vma=False,
    )
```

```python
import functools
import math

import jax
import jax.numpy as jnp
from jax import lax
from jax.experimental import pallas as pl
from jax.experimental.pallas import tpu as pltpu
from jax.sharding import PartitionSpec as P

AXES = ("pb", "ka")
META = 16
LOG2E = math.log2(math.e)


def nt_dot(left, right):
    return lax.dot_general(
        left, right, (((1,), (1,)), ((), ())), preferred_element_type=jnp.float32
    )


def nn_dot(left, right):
    return lax.dot_general(
        left, right, (((1,), (0,)), ((), ())), preferred_element_type=jnp.float32
    )


def pack_kernel(key, value, place, doc, out):
    rows = key.shape[0]
    out[0, :rows, :] = key[...]
    out[0, rows : 2 * rows, :] = value[...]
    index = lax.broadcasted_iota(jnp.int32, (META, rows), 0)
    block = place[0:1, 0:1] // rows
    meta = jnp.where(index == 0, doc[...], block).astype(jnp.float32)
    out[0, 2 * rows :, :] = meta.astype(out.dtype)


def pack(key, value, place, doc):
    rows, head = key.shape
    return pl.pallas_call(
        pack_kernel,
        out_shape=jax.ShapeDtypeStruct((1, 2 * rows + META, head), key.dtype),
        name="pack_rows",
    )(key, value, place, doc)


def stats_kernel(grad, forward, lse, place, doc, out):
    heads, rows = lse.shape
    head = grad.shape[1] // heads
    for h in range(heads):
        part = slice(h * head, (h + 1) * head)
        product = grad[:, part].astype(jnp.float32) * forward[:, part].astype(jnp.float32)
        spot = slice(h * rows, (h + 1) * rows)
        out[0:1, spot] = lse[h : h + 1, :] * LOG2E
        out[1:2, spot] = jnp.sum(product.T, axis=0, keepdims=True)
        out[2:3, spot] = doc[...].astype(jnp.float32)
        out[3:4, spot] = place[...].astype(jnp.float32)


def row_stats(grad, forward, lse, place, doc):
    heads, rows = lse.shape
    return pl.pallas_call(
        stats_kernel,
        out_shape=jax.ShapeDtypeStruct((4, heads * rows), jnp.float32),
        name="row_stats",
    )(grad, forward, lse, place, doc)


def tile_kernel(q_own, q_peer, g_own, g_peer, s_own, s_peer, kv, *rest, last):
    if last:
        dqt_in, dq_own, dq_peer, out, qs, gs, dqt, acc, flags, firsts = rest
        dqt[...] = dqt_in[...]
    else:
        dqt, out, qs, gs, acc, flags, firsts = rest
        dqt[...] = jnp.zeros_like(dqt)
    rows, width = q_own.shape
    slots, span, head = kv.shape
    heads = width // head
    scale = head ** (-0.5)
    stats = (s_own, s_peer)
    places = [s[3:4, :rows][0, 0] for s in stats]
    docs = [s[2:3, :rows][0, 0] for s in stats]
    for slot in range(slots):
        meta = kv[slot, 2 * rows :, :].astype(jnp.float32)
        first = meta[1, 0] * rows
        firsts[slot] = first
        for block in range(2):
            seen = (first <= places[block]) & (meta[0, rows - 1] >= docs[block])
            flags[2 * slot + block] = seen.astype(jnp.int32)
    for block, (q, g) in enumerate(((q_own, g_own), (q_peer, g_peer))):
        for h in range(heads):
            qs[block, h * rows : (h + 1) * rows, :] = q[:, h * head : (h + 1) * head]
            gs[block, h * rows : (h + 1) * rows, :] = g[:, h * head : (h + 1) * head]

    def over_slots(slot, carry):
        acc[...] = jnp.zeros_like(acc)

        for block in range(2):

            @pl.when(flags[2 * slot + block] == 1)
            def _():
                key = kv[slot, :rows, :]
                value = kv[slot, rows : 2 * rows, :]
                doc_row = kv[slot, 2 * rows :, :].astype(jnp.float32)[0:1, :]
                key_t = key.astype(jnp.float32).T.astype(jnp.bfloat16)
                doc_col = jnp.broadcast_to(doc_row, (rows, rows)).T[:, 0:1]
                index = lax.broadcasted_iota(jnp.int32, (rows, 1), 0)
                place_col = index.astype(jnp.float32) + firsts[slot]
                s = stats[block]
                visible = (place_col <= s[3:4, :]) & (doc_col == s[2:3, :])
                scores = nt_dot(key, qs[block])
                weights = jnp.where(
                    visible, jnp.exp2(scores * (scale * LOG2E) - s[0:1, :]), 0.0
                )
                grads = nt_dot(value, gs[block])
                score_grads = (weights * (grads - s[1:2, :])).astype(jnp.bfloat16)
                acc[rows:, :] += nn_dot(weights.astype(jnp.bfloat16), gs[block])
                acc[:rows, :] += nn_dot(score_grads, qs[block])
                dqt[block] += nn_dot(key_t, score_grads)

        out[slot, :rows, :] = (acc[:rows, :] * scale).astype(out.dtype)
        out[slot, rows:, :] = acc[rows:, :].astype(out.dtype)
        return carry

    lax.fori_loop(0, slots, over_slots, 0)
    if last:
        for block, dq in enumerate((dq_own, dq_peer)):
            for h in range(heads):
                dq[:, h * head : (h + 1) * head] = (
                    dqt[block, :, h * rows : (h + 1) * rows].T * scale
                ).astype(dq.dtype)


def tile_grads(operands, kv, dqt=None):
    rows, width = operands[0].shape
    slots, _, head = kv.shape
    heads = width // head
    last = dqt is not None
    dqt_kind = (2, head, heads * rows)
    if last:
        outs = [
            jax.ShapeDtypeStruct((rows, width), jnp.float32),
            jax.ShapeDtypeStruct((rows, width), jnp.bfloat16),
            jax.ShapeDtypeStruct((slots, 2 * rows, head), jnp.float32),
        ]
    else:
        outs = [
            jax.ShapeDtypeStruct(dqt_kind, jnp.float32),
            jax.ShapeDtypeStruct((slots, 2 * rows, head), jnp.bfloat16),
        ]
    stacked = pltpu.VMEM((2, heads * rows, head), jnp.bfloat16)
    flops = 20 * slots * rows * rows * heads * head
    return pl.pallas_call(
        functools.partial(tile_kernel, last=last),
        out_shape=outs,
        scratch_shapes=[stacked, stacked]
        + ([pltpu.VMEM(dqt_kind, jnp.float32)] if last else [])
        + [
            pltpu.VMEM((2 * rows, head), jnp.float32),
            pltpu.SMEM((2 * slots,), jnp.int32),
            pltpu.SMEM((slots,), jnp.float32),
        ],
        cost_estimate=pl.CostEstimate(flops=flops, bytes_accessed=0, transcendentals=0),
        name="tile_grads_kept" if last else "tile_grads_sent",
    )(*operands, kv, *([dqt] if last else []))


def make_body(pb_size, ka_size):
    total = pb_size * ka_size
    core = ka_size
    bits = [1 << b for b in reversed(range(ka_size.bit_length() - 1))]
    bits += [1 << b for b in range(total.bit_length() - 1) if (1 << b) > core]
    orders = (bits, bits[:1] + bits[2:] + bits[1:2])

    def peer(array):
        return lax.ppermute(array, AXES, [(i, i ^ core) for i in range(total)])

    def swap(array, level):
        pairs = [(i, i ^ orders[1 if i & core else 0][level]) for i in range(total)]
        return lax.ppermute(array, AXES, pairs)

    def body(queries, key_rows, value_rows, forward_out, out_grad, logsumexp, position, segment):
        rows = queries.shape[0]
        place, doc = position[None, :], segment[None, :]
        kv = pack(key_rows, value_rows, place, doc)
        stats = row_stats(out_grad, forward_out, logsumexp, place, doc)
        last = len(bits) - 1
        for level in range(last):
            kv = jnp.concatenate([kv, swap(kv, level)])
        kv_high = swap(kv, last)
        q_peer, g_peer, s_peer = peer(queries), peer(out_grad), peer(stats)
        operands = (queries, q_peer, out_grad, g_peer, stats, s_peer)
        dqt, send = tile_grads(operands, kv_high)
        received = swap(send, last)
        dq_own, dq_send, keep = tile_grads(operands, kv, dqt)
        kept = keep + received.astype(jnp.float32)
        dq_recv = peer(dq_send)
        for level in reversed(range(last)):
            half = kept.shape[0] // 2
            keep, send = kept[:half], kept[half:].astype(jnp.bfloat16)
            kept = keep + swap(send, level).astype(jnp.float32)
        query_grad = (dq_own + dq_recv.astype(jnp.float32)).astype(jnp.bfloat16)
        kept = kept[0].astype(jnp.bfloat16)
        return query_grad, kept[:rows], kept[rows:]

    return body


def solution(mesh):
    placed = (
        P(AXES, None),
        P(AXES, None),
        P(AXES, None),
        P(AXES, None),
        P(AXES, None),
        P(None, AXES),
        P(AXES),
        P(AXES),
    )
    return jax.shard_map(
        make_body(mesh.shape["pb"], mesh.shape["ka"]),
        mesh=mesh,
        in_specs=placed,
        out_specs=(P(AXES, None), P(AXES, None), P(AXES, None)),
        check_vma=False,
    )
```
